32 devices in a mesh: members: 2 (over y), stars: 16 (over z, x, core).
Axes of the slice: x: 2, y: 2, z: 4, core: 2. Of those that a mesh axis runs over, the one named last changes fastest.
Arguments:
- position: float32 [3, 8192], P(None, ('members', 'stars')), parts along dimension 1, may hold values from -8 to 8
- velocity: float32 [3, 8192], P(None, ('members', 'stars')), parts along dimension 1, may hold values from -2 to 2
- acceleration: float32 [3, 8192], P(None, ('members', 'stars')), parts along dimension 1, may hold values from -2 to 2
- old_jerk: float32 [3, 8192], P(None, ('members', 'stars')), parts along dimension 1, may hold values from -6 to 6
- masses: float32 [8192], P(('members', 'stars')), parts along dimension 0, may hold values from 4.8828126e-05 to 0.0012207031
- levels: int32 [8192], P(('members', 'stars')), parts along dimension 0, may hold values from 0 to 3
- active_count: int32 [32], P(('members', 'stars')), parts along dimension 0, may hold values from 0 to 32, as said below
- active_slot: int32 [1024], P(('members', 'stars')), parts along dimension 0, may hold values from 0 to 255, as said below
Outputs:
- corrected: float32 [4, 3, 1024], P(None, None, ('members', 'stars')), parts along dimension 2
- derivatives: float32 [2, 3, 1024], P(None, None, ('members', 'stars')), parts along dimension 2
The draws below stay inside these ranges and needn't reach their ends.
There are 2 independent parts, one for each index of `members`. The reference program is written for one: setup_inputs(seed, part) draws one part's arguments, and reference() takes and returns one part's arrays. A program takes and returns all parts, laid end to end along the dimension named above; each array names one. Nothing has to cross between parts.
Inputs may be any that keep to these rules, and one draw needn't show every extreme that they name: `active_count`: the entries sum to 256; some entry equals 32 and some equals 0. `active_slot`: the 32 entries of one group are distinct; only its first active_count entries are live.
All inputs are finite; a program needn't handle non-finite values.
Results may differ from the reference program's by a relative error of at most 0.00002.
Values sent between devices are 32-bit elements; how exact they have to be, the bound alone decides.
No kernel may reach another device: no remote copies, remote signals or barrier semaphores. Data moves between devices by JAX's collectives and lax.ppermute only.
A program may use at most 64 MiB of HBM per device.

```python
import math
import jax
import jax.numpy as jnp
from jax import lax

RES_DEV = 256
CAP = 32
OWNERS = 16
STARS = 4096


def draw_position(key, part):
    key_radius = jax.random.fold_in(key, 11)
    key_direction = jax.random.fold_in(key, 12)
    radius_scale = 0.6
    fraction = jax.random.uniform(key_radius, (STARS,), jnp.float32, 0.001, 0.995)
    radius = radius_scale / jnp.sqrt(jnp.power(fraction, -2.0 / 3.0) - 1.0)
    heading = jax.random.normal(key_direction, (3, STARS), jnp.float32)
    length = jnp.sqrt(jnp.sum(heading * heading, axis=0))
    heading = heading / jnp.maximum(length, 0.001)[None, :]
    placed = jnp.clip(radius[None, :] * heading, -8.0, 8.0)
    return placed.astype(jnp.float32)


def draw_active_count(key, part):
    half = CAP // 2
    shuffle = jax.random.permutation(jax.random.fold_in(key, 21), OWNERS)
    shifts = jax.random.randint(jax.random.fold_in(key, 22), (OWNERS // 2,), 0, half + 1)
    shifts = shifts.at[0].set(half)
    values = jnp.concatenate([half + shifts, half - shifts]).astype(jnp.int32)
    return jnp.zeros((OWNERS,), jnp.int32).at[shuffle].set(values)


def draw_active_slot(key, part):
    group_keys = jax.random.split(jax.random.fold_in(key, 31), OWNERS)

    def one_group(group_key):
        return jax.random.permutation(group_key, RES_DEV)[:CAP]
    return jax.vmap(one_group)(group_keys).reshape(-1).astype(jnp.int32)


def touch_ends(drawn, stream_key, smallest, top_value):
    longest = drawn.shape.index(max(drawn.shape))
    spots = []
    for shift in (0, 1):
        where = [jax.random.randint(jax.random.fold_in(stream_key, axis), (), 0, length) for axis, length in enumerate(drawn.shape)]
        where[longest] = (where[longest] + shift) % drawn.shape[longest]
        spots.append(tuple(where))
    return drawn.at[spots[0]].set(smallest).at[spots[1]].set(top_value)


def block_scale(rng, shape, cuts, low, top_value):
    def one(dim, parts):
        heights = jax.random.uniform(jax.random.fold_in(jax.random.fold_in(rng, 6), dim), (parts,), jnp.float32, low / len(cuts), top_value / len(cuts))
        return jnp.repeat(jnp.exp(heights), shape[dim] // parts).reshape((-1,) + (1,) * (len(shape) - dim - 1))

    gain = one(*cuts[0])
    for cut in cuts[1:]:
        gain = gain * one(*cut)
    return gain


def noise(key, dims, deviation, bound, cuts=(), kind=jnp.bfloat16):
    loudness = block_scale(key, dims, cuts, -0.22, 0.18) if cuts else 1.0
    drawn = jax.random.normal(key, dims, jnp.float32) * deviation * loudness
    return jnp.minimum(jnp.maximum(drawn, -bound), bound).astype(kind)


def setup_inputs(seed: int = 0, part: int = 0) -> dict:
    streams_of = jax.random.split(jax.random.key(seed), 9)
    part_keys = jax.random.split(jax.random.fold_in(streams_of[8], part), 9)
    return {
        "position": draw_position(jax.random.fold_in(jax.random.fold_in(streams_of[8], part), 71), part),
        "velocity": noise(part_keys[1], (3, STARS), 0.3, 2.0, ((1, 16),), jnp.float32),
        "acceleration": noise(part_keys[2], (3, STARS), 0.3, 2.0, ((1, 16),), jnp.float32),
        "old_jerk": noise(part_keys[3], (3, STARS), 1.0, 6.0, ((1, 16),), jnp.float32),
        "masses": jnp.clip(jnp.exp(math.log(0.0012207031) - 3.218876 * jax.random.uniform(part_keys[4], (STARS,), jnp.float32) ** block_scale(part_keys[4], (STARS,), ((0, 16),), -0.2, 0.2)), 4.882812572759576e-05, 0.0012207031),
        "levels": touch_ends(jax.random.randint(part_keys[5], (STARS,), 0, 4), jax.random.fold_in(part_keys[5], 1), 0, 3).astype(jnp.int32),
        "active_count": draw_active_count(jax.random.fold_in(jax.random.fold_in(streams_of[8], part), 71), part),
        "active_slot": draw_active_slot(jax.random.fold_in(jax.random.fold_in(streams_of[8], part), 71), part),
    }


SOFTEN = 0.0025
STEP_BASE = 0.5

def pair_terms(targets, res_pos, res_vel, res_mass):
    separation = res_pos[:, None, :] - targets[0:3, :, None]
    relative = res_vel[:, None, :] - targets[3:6, :, None]
    squared = lax.optimization_barrier(jnp.sum(separation * separation, axis=0)) + SOFTEN
    inverse = lax.rsqrt(squared)
    inverse_sq = inverse * inverse
    weight = res_mass[None, :] * inverse * inverse_sq
    radial = 3.0 * lax.optimization_barrier(jnp.sum(separation * relative, axis=0)) * inverse_sq
    pull = lax.optimization_barrier(jnp.sum(weight[None] * separation, axis=2))
    jerk_sum = lax.optimization_barrier(jnp.sum(weight[None] * (relative - radial[None] * separation), axis=2))
    return jnp.concatenate([pull, jerk_sum], axis=0)

def forces(targets, res_pos, res_vel, res_mass, block_limit):
    row_total = targets.shape[1]
    block_rows = row_total if row_total <= block_limit else math.gcd(row_total, block_limit)
    block_count = row_total // block_rows
    target_tiles = targets.reshape(6, block_count, block_rows).transpose(1, 0, 2)

    def one_tile(tile_cols):
        return pair_terms(tile_cols, res_pos, res_vel, res_mass)
    result = lax.map(one_tile, target_tiles)
    return result.transpose(1, 0, 2).reshape(6, row_total)

def predict(position, velocity, acceleration, old_jerk, levels):
    interval = STEP_BASE * jnp.exp2(-levels.astype(jnp.float32))
    moved_pos = position + interval * (velocity + interval * (0.5 * acceleration + interval * old_jerk / 6.0))
    moved_vel = velocity + interval * (acceleration + 0.5 * interval * old_jerk)
    return (moved_pos, moved_vel)

def correct(start_pos, start_vel, start_acc, start_jerk, new_acc, new_jerk, interval, live):
    end_vel = start_vel + 0.5 * interval * (start_acc + new_acc) + interval * interval * (start_jerk - new_jerk) / 12.0
    end_pos = start_pos + 0.5 * interval * (start_vel + end_vel) + interval * interval * (start_acc - new_acc) / 12.0
    differ = start_acc - new_acc
    snap_term = 3.0 * differ + interval * (start_jerk + 2.0 * new_jerk)
    crackle_term = 2.0 * differ + interval * (start_jerk + new_jerk)
    corrected = jnp.where(live[None, None], jnp.stack([end_pos, end_vel, new_acc, new_jerk]), 0.0)
    derivatives = jnp.where(live[None, None], jnp.stack([snap_term, crackle_term]), 0.0)
    return (corrected, derivatives)

def reference(position, velocity, acceleration, old_jerk, masses, levels, active_count, active_slot):
    owners = active_count.shape[0]
    capacity = active_slot.shape[0] // owners
    resident = position.shape[1] // owners
    slot_total = owners * capacity
    active_total = slot_total // 2
    moved_pos, moved_vel = predict(position, velocity, acceleration, old_jerk, levels)
    live = (jnp.arange(capacity, dtype=jnp.int32)[None, :] < active_count[:, None]).reshape(-1)
    global_index = (jnp.arange(owners, dtype=jnp.int32)[:, None] * resident + active_slot.reshape(owners, capacity)).reshape(-1).astype(jnp.int32)
    order_key = jnp.where(live, 0, slot_total).astype(jnp.int32) + jnp.arange(slot_total, dtype=jnp.int32)
    order_index = jnp.argsort(order_key, stable=True)[:active_total].astype(jnp.int32)
    chosen = global_index[order_index]
    targets = jnp.concatenate([moved_pos[:, chosen], moved_vel[:, chosen]], axis=0)
    summed = forces(targets, moved_pos, moved_vel, masses, 32)
    spread_out = jnp.zeros((6, slot_total), jnp.float32).at[:, order_index].set(summed)
    interval = STEP_BASE * jnp.exp2(-levels[global_index].astype(jnp.float32))
    return correct(position[:, global_index], velocity[:, global_index], acceleration[:, global_index], old_jerk[:, global_index], spread_out[0:3], spread_out[3:6], interval, live)
```

```python
import functools

import jax
import jax.numpy as jnp
from jax import lax
from jax.experimental import pallas as pl
from jax.experimental.pallas import tpu as pltpu
from jax.sharding import PartitionSpec as P

SOFTEN = 0.0025
STEP_BASE = 0.5
LANES = 128
SUBLANES = 8
HIGHEST = lax.Precision.HIGHEST


def step_of(levels):
    return STEP_BASE * jnp.exp2(-levels.astype(jnp.float32))


def predict(pos, vel, acc, jerk, h):
    moved_pos = pos + h * (vel + h * (0.5 * acc + h * jerk * (1.0 / 6.0)))
    moved_vel = vel + h * (acc + 0.5 * h * jerk)
    return moved_pos, moved_vel


def pack_kernel(pos, vel, acc, jerk, mass, level, out):
    moved_pos, moved_vel = predict(pos[...], vel[...], acc[...], jerk[...], step_of(level[...]))
    out[0, 0:3] = moved_pos
    out[0, 3:6] = moved_vel
    out[0, 6:7] = mass[...]
    out[0, 7:8] = jnp.zeros_like(mass[...])


def add_block(stars, index, lane, target, sums):
    def row(c):
        return stars[index, pl.ds(c, 1), pl.ds(lane, LANES)]

    d = [row(c) - target[c] for c in range(3)]
    w = [row(c + 3) - target[c + 3] for c in range(3)]
    squared = (d[0] * d[0] + d[1] * d[1]) + (d[2] * d[2] + SOFTEN)
    inverse = lax.rsqrt(squared)
    inverse_sq = inverse * inverse
    weight = (row(6) * inverse) * inverse_sq
    radial = (d[0] * w[0] + d[1] * w[1] + d[2] * w[2]) * inverse_sq
    pull = [weight * c for c in d]
    return (
        tuple(s + p for s, p in zip(sums[0:3], pull))
        + tuple(s + weight * c for s, c in zip(sums[3:6], w))
        + tuple(s + radial * p for s, p in zip(sums[6:9], pull))
    )


def add_stars(stars_refs, target_ref, sums_in, sums_out):
    for tile in range(target_ref.shape[1] // SUBLANES):
        rows = pl.ds(tile * SUBLANES, SUBLANES)
        target = [target_ref[c, rows] for c in range(6)]
        if sums_in is None:
            sums = (jnp.zeros((SUBLANES, LANES), jnp.float32),) * 9
        else:
            sums = tuple(sums_in[c, rows] for c in range(9))
        for stars in stars_refs:
            pieces = stars.shape[2] // LANES

            def group(g, sums):
                for piece in range(pieces):
                    sums = add_block(stars, g, piece * LANES, target, sums)
                return sums

            sums = lax.fori_loop(0, stars.shape[0], group, sums, unroll=min(4, stars.shape[0]))
        for c in range(9):
            sums_out[c, rows] = sums[c]


def own_kernel(packed, pos, vel, acc, jerk, level, slot, target, start, sums, data, index):
    resident = packed.shape[2]
    capacity = slot.shape[1]
    data[...] = jnp.zeros_like(data)
    data[0:6] = packed[0, 0:6]
    data[8:11] = pos[...]
    data[11:14] = vel[...]
    data[14:17] = acc[...]
    data[17:20] = jerk[...]
    data[20:21] = step_of(level[...])
    index[...] = jnp.full_like(index, -1)
    index[:, 0:capacity] = slot[...]
    chosen = lax.broadcasted_iota(jnp.int32, (resident, index.shape[1]), 0) == index[...]
    picked = jnp.dot(
        data[...], chosen.astype(jnp.float32), precision=HIGHEST, preferred_element_type=jnp.float32
    )
    start[...] = picked[8:24]
    columns = picked[0:8].T
    for c in range(6):
        target[c] = jnp.broadcast_to(columns[0 : target.shape[1], c : c + 1], target.shape[1:])
    add_stars([packed], target, None, sums)


def more_kernel(stars, target, sums_in, sums_out):
    add_stars([stars], target, sums_in, sums_out)


def last_kernel(*refs):
    *stars, target, sums_in, start, count, corrected, derivatives, sums = refs
    add_stars(stars, target, sums_in, sums)
    capacity = corrected.shape[2]
    ones = jnp.ones((SUBLANES, LANES), jnp.float32)

    def total(c):
        return lax.dot_general(
            ones, sums[c], (((1,), (1,)), ((), ())), precision=HIGHEST,
            preferred_element_type=jnp.float32,
        )[0:1, 0:capacity]

    live = lax.broadcasted_iota(jnp.int32, (1, capacity), 1) < count[...]
    h = start[12:13, 0:capacity]
    for c in range(3):
        x0, v0, a0, j0 = (start[3 * k + c : 3 * k + c + 1, 0:capacity] for k in range(4))
        a1 = total(c)
        j1 = total(3 + c) - 3.0 * total(6 + c)
        v1 = v0 + 0.5 * h * (a0 + a1) + h * h * (j0 - j1) * (1.0 / 12.0)
        x1 = x0 + 0.5 * h * (v0 + v1) + h * h * (a0 - a1) * (1.0 / 12.0)
        differ = a0 - a1
        snap = 3.0 * differ + h * (j0 + 2.0 * j1)
        crackle = 2.0 * differ + h * (j0 + j1)
        for k, value in enumerate((x1, v1, a1, j1)):
            corrected[k, c : c + 1] = jnp.where(live, value, 0.0)
        for k, value in enumerate((snap, crackle)):
            derivatives[k, c : c + 1] = jnp.where(live, value, 0.0)


def shaped(*shape):
    return jax.ShapeDtypeStruct(shape, jnp.float32)


def shards(groups, position, velocity, acceleration, old_jerk, masses, levels, active_count, active_slot):
    resident = position.shape[1]
    capacity = active_slot.shape[0]
    padded = -(-capacity // LANES) * LANES
    mass = masses.reshape(1, resident)
    level = levels.reshape(1, resident)
    slot = active_slot.reshape(1, capacity)
    count = active_count.reshape(1, 1)
    state = (position, velocity, acceleration, old_jerk)

    packed = pl.pallas_call(pack_kernel, out_shape=shaped(1, 8, resident), name="pack")(*state, mass, level)

    def swap(block, mask):
        return lax.ppermute(block, "stars", [(i, i ^ mask) for i in range(groups)])

    target, start, sums = pl.pallas_call(
        own_kernel,
        out_shape=(shaped(6, capacity, LANES), shaped(16, padded), shaped(9, capacity, LANES)),
        scratch_shapes=[pltpu.VMEM((24, resident), jnp.float32), pltpu.VMEM((1, padded), jnp.int32)],
        name="own",
    )(packed, *state, level, slot)

    def more(stars, sums):
        return pl.pallas_call(
            more_kernel, out_shape=shaped(9, capacity, LANES), name="more"
        )(stars, target, sums)

    held = packed
    mask = groups // 2
    while mask > 2:
        other = swap(held, mask)
        sums = more(other, sums)
        held = jnp.concatenate([held, other], axis=0)
        mask //= 2
    rest = [swap(held, m) for m in (1, 2, 3) if m < groups]
    return pl.pallas_call(
        last_kernel,
        out_shape=(shaped(4, 3, capacity), shaped(2, 3, capacity)),
        scratch_shapes=[pltpu.VMEM((9, capacity, LANES), jnp.float32)],
        name="last",
    )(*rest, target, sums, start, count)


def solution(mesh):
    groups = mesh.shape["stars"]
    assert groups & (groups - 1) == 0
    wide = P(None, ("members", "stars"))
    flat = P(("members", "stars"))
    out = P(None, None, ("members", "stars"))
    return jax.shard_map(
        functools.partial(shards, groups),
        mesh=mesh,
        in_specs=(wide, wide, wide, wide, flat, flat, flat, flat),
        out_specs=(out, out),
        check_vma=False,
    )
```

```python
import functools

import jax
import jax.numpy as jnp
from jax import lax
from jax.experimental import pallas as pl
from jax.experimental.pallas import tpu as pltpu
from jax.sharding import PartitionSpec as P

SOFTEN = 0.0025
STEP_BASE = 0.5
LANES = 128
SUBLANES = 8
HIGHEST = lax.Precision.HIGHEST


def step_of(levels):
    return STEP_BASE * jnp.exp2(-levels.astype(jnp.float32))


def predict(pos, vel, acc, jerk, h):
    moved_pos = pos + h * (vel + h * (0.5 * acc + h * jerk * (1.0 / 6.0)))
    moved_vel = vel + h * (acc + 0.5 * h * jerk)
    return moved_pos, moved_vel


def pack_kernel(pos, vel, acc, jerk, mass, level, out, data):
    h = step_of(level[...])
    moved_pos, moved_vel = predict(pos[...], vel[...], acc[...], jerk[...], h)
    out[0, 0:3] = moved_pos
    out[0, 3:6] = moved_vel
    out[0, 6:7] = mass[...]
    out[0, 7:8] = h
    data[0:3] = pos[...]
    data[3:6] = vel[...]
    data[6:9] = acc[...]
    data[9:12] = jerk[...]
    data[12:16] = jnp.zeros_like(data[12:16])


def add_block(stars, index, lane, target, sums):
    def row(c):
        return stars[index, pl.ds(c, 1), pl.ds(lane, LANES)]

    d = [row(c) - target[c] for c in range(3)]
    w = [row(c + 3) - target[c + 3] for c in range(3)]
    squared = (d[0] * d[0] + d[1] * d[1]) + (d[2] * d[2] + SOFTEN)
    inverse = lax.rsqrt(squared)
    inverse_sq = inverse * inverse
    weight = (row(6) * inverse) * inverse_sq
    radial = (d[0] * w[0] + d[1] * w[1] + d[2] * w[2]) * inverse_sq
    pull = [weight * c for c in d]
    return (
        tuple(s + p for s, p in zip(sums[0:3], pull))
        + tuple(s + weight * c for s, c in zip(sums[3:6], w))
        + tuple(s + radial * p for s, p in zip(sums[6:9], pull))
    )


def add_stars(stars_refs, target_ref, sums_in, sums_out):
    for tile in range(target_ref.shape[1] // SUBLANES):
        rows = pl.ds(tile * SUBLANES, SUBLANES)
        target = [target_ref[c, rows] for c in range(6)]
        if sums_in is None:
            sums = (jnp.zeros((SUBLANES, LANES), jnp.float32),) * 9
        else:
            sums = tuple(sums_in[c, rows] for c in range(9))
        for stars in stars_refs:
            pieces = stars.shape[2] // LANES

            def group(g, sums):
                for piece in range(pieces):
                    sums = add_block(stars, g, piece * LANES, target, sums)
                return sums

            sums = lax.fori_loop(0, stars.shape[0], group, sums, unroll=min(4, stars.shape[0]))
        for c in range(9):
            sums_out[c, rows] = sums[c]


def own_kernel(packed, data, slot, target, start, sums, index):
    resident = packed.shape[2]
    capacity = slot.shape[1]
    index[...] = jnp.full_like(index, -1)
    index[:, 0:capacity] = slot[...]
    chosen = lax.broadcasted_iota(jnp.int32, (resident, index.shape[1]), 0) == index[...]
    chosen = chosen.astype(jnp.float32)

    def pick(values):
        return jnp.dot(values, chosen, precision=HIGHEST, preferred_element_type=jnp.float32)

    moved = pick(packed[0])
    start[0:16] = pick(data[...])
    start[16:24] = moved
    columns = moved.T
    for c in range(6):
        target[c] = jnp.broadcast_to(columns[0 : target.shape[1], c : c + 1], target.shape[1:])
    add_stars([packed], target, None, sums)


def more_kernel(stars, target, sums_in, sums_out):
    add_stars([stars], target, sums_in, sums_out)


def last_kernel(*refs):
    *stars, target, sums_in, start, count, corrected, derivatives, sums = refs
    add_stars(stars, target, sums_in, sums)
    capacity = corrected.shape[2]
    ones = jnp.ones((SUBLANES, LANES), jnp.float32)

    def total(c):
        return lax.dot_general(
            ones, sums[c], (((1,), (1,)), ((), ())), precision=HIGHEST,
            preferred_element_type=jnp.float32,
        )[0:1, 0:capacity]

    live = lax.broadcasted_iota(jnp.int32, (1, capacity), 1) < count[...]
    h = start[23:24, 0:capacity]
    for c in range(3):
        x0, v0, a0, j0 = (start[3 * k + c : 3 * k + c + 1, 0:capacity] for k in range(4))
        a1 = total(c)
        j1 = total(3 + c) - 3.0 * total(6 + c)
        v1 = v0 + 0.5 * h * (a0 + a1) + h * h * (j0 - j1) * (1.0 / 12.0)
        x1 = x0 + 0.5 * h * (v0 + v1) + h * h * (a0 - a1) * (1.0 / 12.0)
        differ = a0 - a1
        snap = 3.0 * differ + h * (j0 + 2.0 * j1)
        crackle = 2.0 * differ + h * (j0 + j1)
        for k, value in enumerate((x1, v1, a1, j1)):
            corrected[c, k : k + 1] = jnp.where(live, value, 0.0)
        for k, value in enumerate((snap, crackle)):
            derivatives[c, k : k + 1] = jnp.where(live, value, 0.0)


def call(kernel, outs, *args, inside=True, **kwargs):
    space = pltpu.VMEM if inside else jax.ShapeDtypeStruct
    return pl.pallas_call(kernel, out_shape=tuple(space(o, jnp.float32) for o in outs), **kwargs)(*args)


def keep(x):
    return pltpu.with_memory_space_constraint(x, pltpu.VMEM)


def shards(groups, position, velocity, acceleration, old_jerk, masses, levels, active_count, active_slot):
    resident = position.shape[1]
    capacity = active_slot.shape[0]
    padded = -(-capacity // LANES) * LANES
    mass = masses.reshape(1, resident)
    level = levels.reshape(1, resident)
    slot = active_slot.reshape(1, capacity)
    count = active_count.reshape(1, 1)
    packed, data = call(
        pack_kernel, ((1, 8, resident), (16, resident)),
        position, velocity, acceleration, old_jerk, mass, level, name="pack",
    )

    def swap(block, mask):
        return lax.ppermute(block, "stars", [(i, i ^ mask) for i in range(groups)])

    all_sums = (9, capacity, LANES)
    target, start, sums = call(
        own_kernel, ((6, capacity, LANES), (24, padded), all_sums), keep(packed), keep(data), slot,
        scratch_shapes=[pltpu.VMEM((1, padded), jnp.int32)], name="own",
    )
    held = packed
    mask = groups // 2
    while mask > 2:
        other = swap(held, mask)
        (sums,) = call(more_kernel, (all_sums,), keep(other), keep(target), keep(sums), name="more")
        held = jnp.concatenate([held, other], axis=0)
        mask //= 2
    rest = [swap(held, m) for m in (1, 2, 3) if m < groups]
    corrected, derivatives = call(
        last_kernel, ((3, 4, capacity), (3, 2, capacity)),
        *(keep(x) for x in (*rest, target, sums, start)), count, inside=False,
        scratch_shapes=[pltpu.VMEM(all_sums, jnp.float32)], name="last",
    )
    return jnp.swapaxes(corrected, 0, 1), jnp.swapaxes(derivatives, 0, 1)


def solution(mesh):
    groups = mesh.shape["stars"]
    assert groups & (groups - 1) == 0
    wide = P(None, ("members", "stars"))
    flat = P(("members", "stars"))
    out = P(None, None, ("members", "stars"))
    return jax.shard_map(
        functools.partial(shards, groups),
        mesh=mesh,
        in_specs=(wide, wide, wide, wide, flat, flat, flat, flat),
        out_specs=(out, out),
        check_vma=False,
    )
```

```python
import functools

import jax
import jax.numpy as jnp
from jax import lax
from jax.experimental import pallas as pl
from jax.experimental.pallas import tpu as pltpu
from jax.sharding import PartitionSpec as P

SOFTEN = 0.0025
STEP_BASE = 0.5
LANES = 128
SUBLANES = 8
HIGHEST = lax.Precision.HIGHEST


def step_of(levels):
    return STEP_BASE * jnp.exp2(-levels.astype(jnp.float32))


def predict(pos, vel, acc, jerk, h):
    moved_pos = pos + h * (vel + h * (0.5 * acc + h * jerk * (1.0 / 6.0)))
    moved_vel = vel + h * (acc + 0.5 * h * jerk)
    return moved_pos, moved_vel


def pack_kernel(pos, vel, acc, jerk, mass, level, slot, out, data):
    resident = pos.shape[1]
    capacity = slot.shape[0]
    h = step_of(level[...]).reshape(1, resident)
    moved_pos, moved_vel = predict(pos[...], vel[...], acc[...], jerk[...], h)
    out[0, 0:3] = moved_pos
    out[0, 3:6] = moved_vel
    out[0, 6:7] = mass[...].reshape(1, resident)
    out[0, 7:8] = h
    data[0:3] = pos[...]
    data[3:6] = vel[...]
    data[6:9] = acc[...]
    data[9:12] = jerk[...]
    data[12:16] = jnp.full((4, resident), -1.0, jnp.float32)
    data[12:13, 0:capacity] = slot[...].astype(jnp.float32).reshape(1, capacity)


def add_block(stars, index, lane, target, sums):
    def row(c):
        return stars[index, pl.ds(c, 1), pl.ds(lane, LANES)]

    d = [row(c) - target[c] for c in range(3)]
    w = [row(c + 3) - target[c + 3] for c in range(3)]
    squared = (d[0] * d[0] + d[1] * d[1]) + (d[2] * d[2] + SOFTEN)
    inverse = lax.rsqrt(squared)
    inverse_sq = inverse * inverse
    weight = (row(6) * inverse) * inverse_sq
    radial = (d[0] * w[0] + d[1] * w[1] + d[2] * w[2]) * inverse_sq
    pull = [weight * c for c in d]
    return (
        tuple(s + p for s, p in zip(sums[0:3], pull))
        + tuple(s + weight * c for s, c in zip(sums[3:6], w))
        + tuple(s + radial * p for s, p in zip(sums[6:9], pull))
    )


def add_stars(stars_refs, target_ref, sums_in, sums_out):
    for tile in range(target_ref.shape[1] // SUBLANES):
        rows = pl.ds(tile * SUBLANES, SUBLANES)
        target = [target_ref[c, rows] for c in range(6)]
        if sums_in is None:
            sums = (jnp.zeros((SUBLANES, LANES), jnp.float32),) * 9
        else:
            sums = tuple(sums_in[c, rows] for c in range(9))
        for stars in stars_refs:
            pieces = stars.shape[2] // LANES

            def group(g, sums):
                for piece in range(pieces):
                    sums = add_block(stars, g, piece * LANES, target, sums)
                return sums

            sums = lax.fori_loop(0, stars.shape[0], group, sums, unroll=min(4, stars.shape[0]))
        for c in range(9):
            sums_out[c, rows] = sums[c]


def own_kernel(packed, data, target, start, sums):
    resident = packed.shape[2]
    padded = start.shape[1]
    slot = data[12:13, 0:padded].astype(jnp.int32)
    chosen = lax.broadcasted_iota(jnp.int32, (resident, padded), 0) == slot
    chosen = jnp.where(chosen, 1.0, 0.0)

    def pick(values):
        return jnp.dot(values, chosen, precision=HIGHEST, preferred_element_type=jnp.float32)

    moved = pick(packed[0])
    start[0:16] = pick(data[...])
    start[16:24] = moved
    columns = moved.T
    for c in range(6):
        target[c] = jnp.broadcast_to(columns[0 : target.shape[1], c : c + 1], target.shape[1:])
    add_stars([packed], target, None, sums)


def more_kernel(stars, target, sums_in, sums_out):
    add_stars([stars], target, sums_in, sums_out)


def last_kernel(*refs):
    *stars, target, sums_in, start, live_ref, corrected, derivatives, sums = refs
    add_stars(stars, target, sums_in, sums)
    capacity = corrected.shape[2]
    ones = jnp.ones((SUBLANES, LANES), jnp.float32)

    def total(c):
        return lax.dot_general(
            ones, sums[c], (((1,), (1,)), ((), ())), precision=HIGHEST,
            preferred_element_type=jnp.float32,
        )[0:1, 0:capacity]

    live = live_ref[...] > 0.0
    h = start[23:24, 0:capacity]
    for c in range(3):
        x0, v0, a0, j0 = (start[3 * k + c : 3 * k + c + 1, 0:capacity] for k in range(4))
        a1 = total(c)
        j1 = total(3 + c) - 3.0 * total(6 + c)
        v1 = v0 + 0.5 * h * (a0 + a1) + h * h * (j0 - j1) * (1.0 / 12.0)
        x1 = x0 + 0.5 * h * (v0 + v1) + h * h * (a0 - a1) * (1.0 / 12.0)
        differ = a0 - a1
        snap = 3.0 * differ + h * (j0 + 2.0 * j1)
        crackle = 2.0 * differ + h * (j0 + j1)
        for k, value in enumerate((x1, v1, a1, j1)):
            corrected[c, k : k + 1] = jnp.where(live, value, 0.0)
        for k, value in enumerate((snap, crackle)):
            derivatives[c, k : k + 1] = jnp.where(live, value, 0.0)


def call(kernel, outs, *args, inside=True, **kwargs):
    space = pltpu.VMEM if inside else jax.ShapeDtypeStruct
    return pl.pallas_call(kernel, out_shape=tuple(space(o, jnp.float32) for o in outs), **kwargs)(*args)


def keep(x):
    return pltpu.with_memory_space_constraint(x, pltpu.VMEM)


def shards(groups, position, velocity, acceleration, old_jerk, masses, levels, active_count, active_slot):
    resident = position.shape[1]
    capacity = active_slot.shape[0]
    padded = -(-capacity // LANES) * LANES
    assert padded <= resident
    packed, data = call(
        pack_kernel, ((1, 8, resident), (16, resident)),
        position, velocity, acceleration, old_jerk, masses, levels, active_slot, name="pack",
    )

    def swap(block, mask):
        return lax.ppermute(block, "stars", [(i, i ^ mask) for i in range(groups)])

    all_sums = (9, capacity, LANES)

    def more(stars, sums):
        return call(more_kernel, (all_sums,), keep(stars), keep(target), keep(sums), name="more")[0]

    target, start, sums = call(
        own_kernel, ((6, capacity, LANES), (24, padded), all_sums), keep(packed), keep(data), name="own",
    )
    slots = lax.broadcasted_iota(jnp.int32, (1, capacity), 1)
    live = active_count
    held = packed
    mask = groups // 2
    while mask > 1:
        other = swap(held, mask | 1)
        if mask == 2:
            early = swap(held, 1)
        other, sums, live = lax.optimization_barrier((other, sums, live))
        if mask == groups // 2:
            live = jnp.where(slots < live, 1.0, 0.0)
        if mask == 2:
            late = swap(other, 1)
            sums = more(early, sums)
        sums = more(other, sums)
        held = jnp.concatenate([held, other], axis=0)
        mask //= 2
    corrected, derivatives = call(
        last_kernel, ((3, 4, capacity), (3, 2, capacity)),
        *(keep(x) for x in (late, target, sums, start, live)), inside=False,
        scratch_shapes=[pltpu.VMEM(all_sums, jnp.float32)], name="last",
    )
    return jnp.swapaxes(corrected, 0, 1), jnp.swapaxes(derivatives, 0, 1)


def solution(mesh):
    groups = mesh.shape["stars"]
    assert groups & (groups - 1) == 0
    wide = P(None, ("members", "stars"))
    flat = P(("members", "stars"))
    out = P(None, None, ("members", "stars"))
    return jax.shard_map(
        functools.partial(shards, groups),
        mesh=mesh,
        in_specs=(wide, wide, wide, wide, flat, flat, flat, flat),
        out_specs=(out, out),
        check_vma=False,
    )
```
